32 devices in a mesh: row: 4 (over y, x), col: 8 (over z, core).
Axes of the slice: x: 2, y: 2, z: 4, core: 2. Of those that a mesh axis runs over, the one named last changes fastest.
Arguments:
- pixels: bfloat16 [64, 16000, 144], P(None, ('row', 'col')), may hold values from 0.049804688 to 4
- match_filter: bfloat16 [16000, 2, 144], P(('row', 'col')), may hold values from -48 to 48
- tile_ranks: int32 [32, 64], P('row', 'col'), may hold values from 1 to 64
- column_order: int32 [64], replicated, may hold values from 0 to 63, each once
- right_factors: bfloat16 [32, 64, 64, 500], P('row', 'col'), may hold values from -0.25 to 0.25
- left_factors: bfloat16 [32, 64, 64, 500], P('row', 'col'), may hold values from -0.09375 to 0.09375
Outputs:
- commands: float32 [64, 16000], P(None, ('row', 'col'))
The draws below stay inside these ranges and needn't reach their ends.
Inputs may be any that keep to these rules, and one draw needn't show every extreme that they name: `column_order`: every slope block is read by exactly one tile column.
All inputs are finite; a program needn't handle non-finite values.
Results may differ from the reference program's by a relative error of at most 0.0041.
Values may be sent and summed in bfloat16 or wider, within the bound.
No kernel may reach another device: no remote copies, remote signals or barrier semaphores. Data moves between devices by JAX's collectives and lax.ppermute only.
A program may use at most 128 MiB of HBM per device.

```python
import math
import jax
import jax.numpy as jnp
from jax import lax

PIX = 144
TILE = 500
RMAX = 64
FRAMES = 64
TCOLS = 64
TROWS = 32
SUBAPS = 16000
SLOPES = 32000
ACT = 16000


def touch_ends(values, stream_key, low, high):
    longest = values.shape.index(max(values.shape))
    spots = []
    for shift in (0, 1):
        where = [jax.random.randint(jax.random.fold_in(stream_key, axis), (), 0, length) for axis, length in enumerate(values.shape)]
        where[longest] = (where[longest] + shift) % values.shape[longest]
        spots.append(tuple(where))
    return values.at[spots[0]].set(low).at[spots[1]].set(high)


def steps_of(rng, extent, shards, smallest, largest):
    level, own = 1.0, jax.random.fold_in(rng, 6)
    for dim, blocks in shards:
        steps = jnp.exp(jax.random.uniform(jax.random.fold_in(own, dim), (blocks,), jnp.float32, smallest / len(shards), largest / len(shards)))
        level = level * jnp.repeat(steps, extent[dim] // blocks).reshape([-1 if axis == dim else 1 for axis in range(len(extent))])
    return level


def scatter_about(rng, extent, deviation, limit, cuts=(), kind=jnp.bfloat16):
    factor_of = steps_of(rng, extent, cuts, -0.22, 0.18) if cuts else 1.0
    result = jax.random.normal(rng, extent, jnp.float32) * deviation * factor_of
    return jnp.minimum(jnp.maximum(result, -limit), limit).astype(kind)


def setup_inputs(seed: int = 0) -> dict:
    keys = jax.random.split(jax.random.key(seed), 7)
    return {
        "pixels": jnp.clip(jnp.exp(math.log(4.0) - 4.3859405 * jax.random.uniform(keys[0], (FRAMES, SUBAPS, PIX), jnp.float32) ** steps_of(keys[0], (FRAMES, SUBAPS, PIX), ((1, 32),), -0.2, 0.2)), 0.049804688, 4.0).astype(jnp.bfloat16),
        "match_filter": scatter_about(keys[1], (SUBAPS, 2, PIX), 8.0, 48.0, ((0, 32),)),
        "tile_ranks": touch_ends(jax.random.randint(keys[2], (TROWS, TCOLS), 1, RMAX + 1), jax.random.fold_in(keys[2], 1), 1, RMAX).astype(jnp.int32),
        "column_order": jax.random.permutation(keys[3], TCOLS).astype(jnp.int32),
        "right_factors": scatter_about(keys[4], (TROWS, TCOLS, RMAX, TILE), TILE ** -0.5, 0.25, ((0, 4), (1, 8))),
        "left_factors": scatter_about(keys[5], (TROWS, TCOLS, RMAX, TILE), (RMAX * TCOLS) ** -0.5, 0.09375, ((0, 4), (1, 8))),
    }


def reference(pixels, match_filter, tile_ranks, column_order, right_factors, left_factors):
    filters_wide = match_filter.astype(jnp.float32)

    def centroid(frame_pixels):
        values = frame_pixels.astype(jnp.float32)
        flux = jnp.sum(values, axis=1)
        raw = jnp.einsum('sp,skp->sk', values, filters_wide)
        return (raw / flux[:, None]).astype(jnp.bfloat16).reshape(SLOPES)

    slopes = lax.map(centroid, pixels)
    blocks = slopes.reshape(FRAMES, TCOLS, TILE)
    picked = jnp.take(blocks, column_order, axis=1).astype(jnp.float32)
    component = jnp.arange(RMAX, dtype=jnp.int32)

    def tile_row(inputs):
        right_row, left_row, rank_row = inputs
        projection = jnp.einsum('jkt,fjt->jkf', right_row.astype(jnp.float32), picked)
        keep = component[None, :] < rank_row[:, None]
        projection = jnp.where(keep[:, :, None], projection, 0.0).astype(jnp.bfloat16)
        return jnp.einsum('jkf,jka->fa', projection.astype(jnp.float32), left_row.astype(jnp.float32))

    rows_out = lax.map(tile_row, (right_factors, left_factors, tile_ranks))
    return jnp.transpose(rows_out, (1, 0, 2)).reshape(FRAMES, ACT)
```

```python
import functools

import jax
import jax.numpy as jnp
from jax import lax
from jax.experimental import pallas as pl
from jax.experimental.pallas import tpu as pltpu
from jax.sharding import PartitionSpec as P

F32 = jnp.float32
BF16 = jnp.bfloat16


def centroid_kernel(pix_ref, mf_ref, out_ref, filt, xs, ys, *, per_step, block_count, tile_width, group):
    step = pl.program_id(0)
    pixel_count, width = pix_ref.shape[1], pix_ref.shape[2]
    lanes = filt.shape[2]

    @pl.when(step == 0)
    def _():
        for k in range(2):
            filt[k, :, 0:width] = mf_ref[k].astype(F32)

    rows = 8
    for f0 in range(0, per_step, group):
        for lane in range(0, lanes, 128):
            w = min(128, width - lane)
            cols = slice(lane, lane + w)
            flux = [jnp.zeros((rows, w), F32) for _ in range(group)]
            sx = [jnp.zeros((rows, w), F32) for _ in range(group)]
            sy = [jnp.zeros((rows, w), F32) for _ in range(group)]
            for p in range(0, pixel_count, rows):
                m0 = filt[0, p : p + rows, cols]
                m1 = filt[1, p : p + rows, cols]
                for f in range(group):
                    v = pix_ref[f0 + f, p : p + rows, cols].astype(F32)
                    flux[f] = flux[f] + v
                    sx[f] = sx[f] + v * m0
                    sy[f] = sy[f] + v * m1
            fl = jnp.concatenate([jnp.sum(a, axis=0, keepdims=True) for a in flux], axis=0)
            vx = jnp.concatenate([jnp.sum(a, axis=0, keepdims=True) for a in sx], axis=0)
            vy = jnp.concatenate([jnp.sum(a, axis=0, keepdims=True) for a in sy], axis=0)
            at = pl.ds(pl.multiple_of(step * per_step + f0, group), group)
            xs[at, cols] = vx / fl
            ys[at, cols] = vy / fl

    @pl.when(step == pl.num_programs(0) - 1)
    def _():
        r = lax.broadcasted_iota(jnp.int32, (256, 256), 0)
        c = lax.broadcasted_iota(jnp.int32, (256, 256), 1)
        weave = (c == jnp.where(r < 128, 2 * r, 2 * (r - 128) + 1)).astype(BF16)
        lane_ok = lax.broadcasted_iota(jnp.int32, xs.shape, 1) < width
        x = jnp.where(lane_ok, xs[...], 0.0).astype(BF16)
        y = jnp.where(lane_ok, ys[...], 0.0).astype(BF16)
        parts = []
        for lane in range(0, lanes, 128):
            both = jnp.concatenate([x[:, lane : lane + 128], y[:, lane : lane + 128]], axis=1)
            parts.append(jnp.dot(both, weave, preferred_element_type=F32))
        woven = jnp.concatenate(parts, axis=1)
        chunk = out_ref.shape[1] // block_count
        for b in range(block_count):
            blk = woven[:, b * tile_width : (b + 1) * tile_width].astype(BF16)
            for q in range(out_ref.shape[0]):
                out_ref[q, b * chunk : (b + 1) * chunk, :] = blk[q * chunk : (q + 1) * chunk, :]


def centroid(pixels, match_filter, pieces, tile_width):
    frames, subaps, pixel_count = pixels.shape
    pix = jnp.transpose(pixels, (0, 2, 1))
    filt = jnp.transpose(match_filter, (1, 2, 0))
    per_step = 8
    lanes = -(-subaps // 128) * 128
    block_count = 2 * subaps // tile_width
    body = functools.partial(
        centroid_kernel, per_step=per_step, block_count=block_count, tile_width=tile_width, group=8
    )
    return pl.pallas_call(
        body,
        grid=(frames // per_step,),
        in_specs=[
            pl.BlockSpec((per_step, pixel_count, subaps), lambda s: (s, 0, 0)),
            pl.BlockSpec((2, pixel_count, subaps), lambda s: (0, 0, 0)),
        ],
        out_specs=pl.BlockSpec((pieces, block_count * frames // pieces, tile_width), lambda s: (0, 0, 0)),
        out_shape=jax.ShapeDtypeStruct((pieces, block_count * frames // pieces, tile_width), BF16),
        scratch_shapes=[
            pltpu.VMEM((2, pixel_count, lanes), F32),
            pltpu.VMEM((frames, lanes), F32),
            pltpu.VMEM((frames, lanes), F32),
        ],
        compiler_params=pltpu.CompilerParams(dimension_semantics=("arbitrary",)),
        name="centroid",
    )(pix, filt)


def select_kernel(order, in_ref, out_ref, wide, dest, *, block_count):
    chunk = in_ref.shape[1] // block_count
    wide[...] = in_ref[...].astype(F32)
    dests = out_ref.shape[0]
    span = out_ref.shape[1] // chunk
    for d in range(dests):
        for j in range(span):
            g = order[d * span + j]
            src = g // block_count
            b = g - src * block_count
            for f in range(chunk):
                dest[d, f * span + j : f * span + j + 1, :] = wide[src, pl.ds(b * chunk + f, 1), :]
    out_ref[...] = dest[...].astype(BF16)


def select(order, pieces, dests, block_count):
    rows = pieces.shape[0] * pieces.shape[1] // dests
    width = pieces.shape[2]
    return pl.pallas_call(
        functools.partial(select_kernel, block_count=block_count),
        in_specs=[pl.BlockSpec(memory_space=pltpu.SMEM), pl.BlockSpec(memory_space=pltpu.VMEM)],
        out_specs=pl.BlockSpec(memory_space=pltpu.VMEM),
        out_shape=jax.ShapeDtypeStruct((dests, rows, width), BF16),
        scratch_shapes=[pltpu.VMEM(pieces.shape, F32), pltpu.VMEM((dests, rows, width), F32)],
        name="select",
    )(order, pieces)


def spread_kernel(in_ref, out_ref, wide):
    span, frames, width = out_ref.shape
    for n in range(wide.shape[0]):
        w = min(128, width - 128 * n)
        wide[n, :, 0:w] = in_ref[:, 128 * n : 128 * n + w].astype(F32)
        for j in range(span):
            got = wide[n, pl.ds(j, frames, stride=span), :].astype(BF16)
            out_ref[j, :, 128 * n : 128 * n + w] = got[:, 0:w]


def spread(gathered, span):
    rows, width = gathered.shape
    return pl.pallas_call(
        spread_kernel,
        in_specs=[pl.BlockSpec(memory_space=pltpu.VMEM)],
        out_specs=pl.BlockSpec(memory_space=pltpu.VMEM),
        out_shape=jax.ShapeDtypeStruct((span, rows // span, width), BF16),
        scratch_shapes=[pltpu.VMEM((-(-width // 128), rows, 128), F32)],
        name="spread",
    )(gathered)


def tomo_kernel(index, ranks, picked_ref, right_ref, left_ref, out_ref, proj, *, count):
    rows, span, bound, _ = right_ref.shape
    frames = picked_ref.shape[1]
    component = lax.broadcasted_iota(jnp.int32, (bound, frames), 0)
    for m in range(count):
        i = index[m]
        for j in range(span):
            p = lax.dot_general(
                right_ref[i, j], picked_ref[j], (((1,), (1,)), ((), ())), preferred_element_type=F32
            )
            p = jnp.where(component < ranks[i, j], p, 0.0)
            proj[j * bound : (j + 1) * bound, :] = p.astype(BF16)
        left = left_ref[i].reshape(span * bound, left_ref.shape[3])
        out_ref[m] = lax.dot_general(
            proj[...], left, (((0,), (0,)), ((), ())), preferred_element_type=F32
        ).astype(out_ref.dtype)


def tomo(index, ranks, picked, right, left, dtype):
    count = index.shape[0]
    _, span, bound, width = right.shape
    frames = picked.shape[1]
    vmem = pl.BlockSpec(memory_space=pltpu.VMEM)
    smem = pl.BlockSpec(memory_space=pltpu.SMEM)
    return pl.pallas_call(
        functools.partial(tomo_kernel, count=count),
        in_specs=[smem, smem, vmem, vmem, vmem],
        out_specs=vmem,
        out_shape=jax.ShapeDtypeStruct((count, frames, left.shape[3]), dtype),
        scratch_shapes=[pltpu.VMEM((span * bound, frames), BF16)],
        name="tomo",
    )(index, ranks, picked, right, left)


def add_kernel(own_ref, other_ref, out_ref):
    out_ref[...] = own_ref[...] + other_ref[...].astype(F32)


def route_start(slopes, column_order, span, tile_width, col_count):
    frame_count = slopes.shape[1]
    block_count = slopes.shape[0]
    inverse = jnp.argsort(column_order, stable=True)
    row_index = lax.axis_index("row")
    col_index = lax.axis_index("col")
    device_rank = row_index * col_count + col_index
    block_ids = device_rank * block_count + jnp.arange(block_count, dtype=jnp.int32)
    target = jnp.take(inverse, block_ids) // span
    selector = (jnp.arange(col_count, dtype=jnp.int32)[:, None] == target[None, :]).astype(BF16)
    outgoing = selector[:, :, None, None] * slopes[None]
    received = lax.all_to_all(outgoing, "col", split_axis=0, concat_axis=0, tiled=True)
    source_ids = (
        (row_index * col_count + jnp.arange(col_count, dtype=jnp.int32))[:, None] * block_count
        + jnp.arange(block_count, dtype=jnp.int32)[None, :]
    ).reshape(-1)
    local_slot = jnp.take(inverse, source_ids) - col_index * span
    placement = (jnp.arange(span, dtype=jnp.int32)[:, None] == local_slot[None, :]).astype(BF16)
    flat_blocks = received.reshape(col_count * block_count, frame_count * tile_width)
    placed = jnp.dot(placement, flat_blocks, preferred_element_type=F32)
    return lax.psum(placed.astype(BF16), "row").reshape(span, frame_count, tile_width)


def shards(pixels, match_filter, tile_ranks, column_order, right_factors, left_factors):
    frames = pixels.shape[0]
    rows_mine, span, _, tile_width = right_factors.shape
    row_count = lax.axis_size("row")
    col_count = lax.axis_size("col")
    devices = row_count * col_count
    block_count = 2 * pixels.shape[1] // tile_width

    if frames % devices == 0:
        pieces = centroid(pixels, match_filter, devices, tile_width)
        pieces = lax.all_to_all(pieces, ("row", "col"), split_axis=0, concat_axis=0, tiled=True)
        outgoing = select(column_order, pieces, col_count, block_count)
        mine = lax.all_to_all(outgoing, "col", split_axis=0, concat_axis=0, tiled=True)
        gathered = lax.all_gather(mine, "row", axis=0, tiled=True)
        picked = spread(gathered.reshape(-1, tile_width), span)
    else:
        slopes = centroid(pixels, match_filter, 1, tile_width)
        slopes = slopes.reshape(block_count, frames, tile_width)
        picked = route_start(slopes, column_order, span, tile_width, col_count)

    chips = col_count // 2
    core = lax.axis_index("col") % 2
    chip = lax.axis_index("col") // 2
    actuators = rows_mine * left_factors.shape[3] // col_count
    if rows_mine == col_count:
        pairs = 2 * jnp.arange(chips, dtype=jnp.int32)
        theirs = tomo(pairs + (1 - core), tile_ranks, picked, right_factors, left_factors, BF16)
        received = lax.ppermute(theirs, "col", [(d, d ^ 1) for d in range(col_count)])
        ours = tomo(pairs + core, tile_ranks, picked, right_factors, left_factors, F32)
    else:
        every = tomo(jnp.arange(rows_mine, dtype=jnp.int32), tile_ranks, picked, right_factors, left_factors, F32)
        every = jnp.transpose(every, (1, 0, 2)).reshape(frames, chips, 2, actuators)
        every = jnp.transpose(every, (2, 1, 0, 3))
        theirs = lax.dynamic_index_in_dim(every, 1 - core, 0, keepdims=False).astype(BF16)
        received = lax.ppermute(theirs, "col", [(d, d ^ 1) for d in range(col_count)])
        ours = lax.dynamic_index_in_dim(every, core, 0, keepdims=False)
    total = ours + received.astype(F32)
    out = lax.dynamic_index_in_dim(total, chip, 0, keepdims=False)
    arrived = []
    for m in range(1, chips):
        piece = lax.dynamic_index_in_dim(total, (chip + m) % chips, 0, keepdims=False).astype(BF16)
        arrived.append(lax.ppermute(piece, "col", [(d, (d + 2 * m) % col_count) for d in range(col_count)]))
    for a in arrived:
        out = out + a.astype(F32)
    return out


def solution(mesh):
    in_specs = (
        P(None, ("row", "col"), None),
        P(("row", "col"), None, None),
        P("row", "col"),
        P(),
        P("row", "col", None, None),
        P("row", "col", None, None),
    )
    out_specs = P(None, ("row", "col"))
    return jax.shard_map(shards, mesh=mesh, in_specs=in_specs, out_specs=out_specs, check_vma=False)
```

```python
import functools

import jax
import jax.numpy as jnp
from jax import lax
from jax.experimental import pallas as pl
from jax.experimental.pallas import tpu as pltpu
from jax.sharding import PartitionSpec as P

F32 = jnp.float32
BF16 = jnp.bfloat16


def in_vmem(x):
    return pltpu.with_memory_space_constraint(x, pltpu.VMEM)


def in_hbm(x):
    return pltpu.with_memory_space_constraint(x, pltpu.HBM)


def limit(mib):
    return pltpu.CompilerParams(vmem_limit_bytes=mib << 20)


VMEM = pl.BlockSpec(memory_space=pltpu.VMEM)
SMEM = pl.BlockSpec(memory_space=pltpu.SMEM)
HBM = pl.BlockSpec(memory_space=pltpu.HBM)
GROUP = 8


def centroid_kernel(pix_hbm, mf_ref, out_ref, pix, filt, xs, ys, sems, *, block_count, tile_width):
    frames, pixel_count, width = pix.shape
    lanes = filt.shape[2]
    steps = frames // GROUP

    def fetch(step):
        at = pl.ds(step * GROUP, GROUP)
        return pltpu.make_async_copy(pix_hbm.at[at], pix.at[at], sems.at[step])

    for step in range(steps):
        fetch(step).start()
    for k in range(2):
        filt[k, :, 0:width] = mf_ref[k].astype(F32)

    rows = 8

    @pl.loop(0, steps)
    def _(step):
        fetch(step).wait()
        f0 = pl.multiple_of(step * GROUP, GROUP)
        for lane in range(0, lanes, 128):
            w = min(128, width - lane)
            cols = slice(lane, lane + w)
            flux = [jnp.zeros((rows, w), F32) for _ in range(GROUP)]
            sx = [jnp.zeros((rows, w), F32) for _ in range(GROUP)]
            sy = [jnp.zeros((rows, w), F32) for _ in range(GROUP)]
            for p in range(0, pixel_count, rows):
                m0 = filt[0, p : p + rows, cols]
                m1 = filt[1, p : p + rows, cols]
                for f in range(GROUP):
                    v = pix[f0 + f, p : p + rows, cols].astype(F32)
                    flux[f] = flux[f] + v
                    sx[f] = sx[f] + v * m0
                    sy[f] = sy[f] + v * m1
            fl = jnp.concatenate([jnp.sum(a, axis=0, keepdims=True) for a in flux], axis=0)
            vx = jnp.concatenate([jnp.sum(a, axis=0, keepdims=True) for a in sx], axis=0)
            vy = jnp.concatenate([jnp.sum(a, axis=0, keepdims=True) for a in sy], axis=0)
            xs[pl.ds(f0, GROUP), cols] = vx / fl
            ys[pl.ds(f0, GROUP), cols] = vy / fl

    r = lax.broadcasted_iota(jnp.int32, (256, 256), 0)
    c = lax.broadcasted_iota(jnp.int32, (256, 256), 1)
    weave = (c == jnp.where(r < 128, 2 * r, 2 * (r - 128) + 1)).astype(BF16)
    lane_ok = lax.broadcasted_iota(jnp.int32, xs.shape, 1) < width
    x = jnp.where(lane_ok, xs[...], 0.0).astype(BF16)
    y = jnp.where(lane_ok, ys[...], 0.0).astype(BF16)
    parts = []
    for lane in range(0, lanes, 128):
        both = jnp.concatenate([x[:, lane : lane + 128], y[:, lane : lane + 128]], axis=1)
        parts.append(jnp.dot(both, weave, preferred_element_type=F32))
    woven = jnp.concatenate(parts, axis=1)
    chunk = out_ref.shape[1] // block_count
    for b in range(block_count):
        blk = woven[:, b * tile_width : (b + 1) * tile_width].astype(BF16)
        for q in range(out_ref.shape[0]):
            out_ref[q, b * chunk : (b + 1) * chunk, :] = blk[q * chunk : (q + 1) * chunk, :]


def centroid(pixels, match_filter, pieces, tile_width):
    frames, subaps, pixel_count = pixels.shape
    pix = jnp.transpose(pixels, (0, 2, 1))
    filt = jnp.transpose(match_filter, (1, 2, 0))
    lanes = -(-subaps // 128) * 128
    block_count = 2 * subaps // tile_width
    return pl.pallas_call(
        functools.partial(centroid_kernel, block_count=block_count, tile_width=tile_width),
        in_specs=[HBM, VMEM],
        out_specs=VMEM,
        out_shape=pltpu.VMEM((pieces, block_count * frames // pieces, tile_width), BF16),
        scratch_shapes=[
            pltpu.VMEM((frames, pixel_count, subaps), BF16),
            pltpu.VMEM((2, pixel_count, lanes), F32),
            pltpu.VMEM((frames, lanes), F32),
            pltpu.VMEM((frames, lanes), F32),
            pltpu.SemaphoreType.DMA((frames // GROUP,)),
        ],
        compiler_params=limit(16),
        name="centroid",
    )(in_hbm(pix), in_hbm(filt))


def select_kernel(order, in_ref, out_ref, wide, dest, *, block_count):
    chunk = in_ref.shape[1] // block_count
    wide[...] = in_ref[...].astype(F32)
    dests = out_ref.shape[0]
    span = out_ref.shape[1] // chunk
    for d in range(dests):
        for j in range(span):
            g = order[d * span + j]
            src = g // block_count
            b = g - src * block_count
            for f in range(chunk):
                dest[d, f * span + j : f * span + j + 1, :] = wide[src, pl.ds(b * chunk + f, 1), :]
    out_ref[...] = dest[...].astype(BF16)


def select(order, pieces, dests, block_count):
    rows = pieces.shape[0] * pieces.shape[1] // dests
    width = pieces.shape[2]
    return pl.pallas_call(
        functools.partial(select_kernel, block_count=block_count),
        in_specs=[SMEM, VMEM],
        out_specs=VMEM,
        out_shape=pltpu.VMEM((dests, rows, width), BF16),
        scratch_shapes=[pltpu.VMEM(pieces.shape, F32), pltpu.VMEM((dests, rows, width), F32)],
        compiler_params=limit(4),
        name="select",
    )(order, in_vmem(pieces))


def spread_kernel(in_ref, out_ref, wide):
    span, width, frames = out_ref.shape
    for n in range(wide.shape[0]):
        w = min(128, width - 128 * n)
        wide[n, :, 0:w] = in_ref[:, 128 * n : 128 * n + w].astype(F32)
        for j in range(span):
            got = jnp.transpose(wide[n, pl.ds(j, frames, stride=span), :]).astype(BF16)
            out_ref[j, 128 * n : 128 * n + w, :] = got[0:w]


def spread(gathered, span):
    rows, width = gathered.shape
    return pl.pallas_call(
        spread_kernel,
        in_specs=[VMEM],
        out_specs=VMEM,
        out_shape=pltpu.VMEM((span, width, rows // span), BF16),
        scratch_shapes=[pltpu.VMEM((-(-width // 128), rows, 128), F32)],
        compiler_params=limit(4),
        name="spread",
    )(in_vmem(gathered))


def tomo_kernel(ranks, picked_ref, right_ref, left_ref, out_ref, proj, *, pick):
    count = out_ref.shape[0]
    _, span, bound, _ = right_ref.shape
    frames = picked_ref.shape[2]
    component = lax.broadcasted_iota(jnp.int32, (bound, frames), 0)
    index = [pick(m) for m in range(count)]
    for j in range(span):
        right = jnp.concatenate([right_ref[i, j] for i in index], axis=0)
        p = jnp.dot(right, picked_ref[j], preferred_element_type=F32)
        for m, i in enumerate(index):
            q = jnp.where(component < ranks[i, j], p[m * bound : (m + 1) * bound], 0.0)
            proj[m, j * bound : (j + 1) * bound, :] = q.astype(BF16)
    for m, i in enumerate(index):
        left = left_ref[i].reshape(span * bound, left_ref.shape[3])
        out_ref[m] = lax.dot_general(
            proj[m], left, (((0,), (0,)), ((), ())), preferred_element_type=F32
        ).astype(out_ref.dtype)


def tomo(pick, count, ranks, picked, right, left, dtype):
    _, span, bound, _ = right.shape
    frames = picked.shape[2]
    return pl.pallas_call(
        functools.partial(tomo_kernel, pick=pick),
        in_specs=[SMEM, VMEM, VMEM, VMEM],
        out_specs=VMEM,
        out_shape=pltpu.VMEM((count, frames, left.shape[3]), dtype),
        scratch_shapes=[pltpu.VMEM((count, span * bound, frames), BF16)],
        compiler_params=limit(8),
        name="tomo",
    )(ranks, in_vmem(picked), in_vmem(right), in_vmem(left))


def own_core():
    return lax.rem(lax.axis_index("col"), 2)


def merge_kernel(own_ref, other_ref, out_ref, *send_refs):
    chips = own_ref.shape[0]
    chip = lax.div(lax.axis_index("col"), 2)
    out_ref[...] = own_ref[chip] + other_ref[chip].astype(F32)
    for m, send in enumerate(send_refs):
        at = lax.rem(chip + m + 1, chips)
        send[...] = (own_ref[at] + other_ref[at].astype(F32)).astype(BF16)


def merge(own, other):
    chips, frames, width = own.shape
    return pl.pallas_call(
        merge_kernel,
        in_specs=[VMEM, VMEM],
        out_specs=[VMEM] * chips,
        out_shape=[pltpu.VMEM((frames, width), F32)] + [pltpu.VMEM((frames, width), BF16)] * (chips - 1),
        compiler_params=limit(4),
        name="merge",
    )(in_vmem(own), in_vmem(other))


def route_start(slopes, column_order, span, tile_width, col_count):
    frame_count = slopes.shape[1]
    block_count = slopes.shape[0]
    inverse = jnp.argsort(column_order, stable=True)
    row_index = lax.axis_index("row")
    col_index = lax.axis_index("col")
    device_rank = row_index * col_count + col_index
    block_ids = device_rank * block_count + jnp.arange(block_count, dtype=jnp.int32)
    target = jnp.take(inverse, block_ids) // span
    selector = (jnp.arange(col_count, dtype=jnp.int32)[:, None] == target[None, :]).astype(BF16)
    outgoing = selector[:, :, None, None] * slopes[None]
    received = lax.all_to_all(outgoing, "col", split_axis=0, concat_axis=0, tiled=True)
    source_ids = (
        (row_index * col_count + jnp.arange(col_count, dtype=jnp.int32))[:, None] * block_count
        + jnp.arange(block_count, dtype=jnp.int32)[None, :]
    ).reshape(-1)
    local_slot = jnp.take(inverse, source_ids) - col_index * span
    placement = (jnp.arange(span, dtype=jnp.int32)[:, None] == local_slot[None, :]).astype(BF16)
    flat_blocks = received.reshape(col_count * block_count, frame_count * tile_width)
    placed = jnp.dot(placement, flat_blocks, preferred_element_type=F32)
    return lax.psum(placed.astype(BF16), "row").reshape(span, frame_count, tile_width)


def shards(pixels, match_filter, tile_ranks, column_order, right_factors, left_factors):
    frames = pixels.shape[0]
    rows_mine, span, _, tile_width = right_factors.shape
    row_count = lax.axis_size("row")
    col_count = lax.axis_size("col")
    devices = row_count * col_count
    block_count = 2 * pixels.shape[1] // tile_width

    if frames % devices == 0:
        pieces = centroid(pixels, match_filter, devices, tile_width)
        pieces = lax.all_to_all(pieces, ("row", "col"), split_axis=0, concat_axis=0, tiled=True)
        outgoing = select(column_order, pieces, col_count, block_count)
        mine = lax.all_to_all(outgoing, "col", split_axis=0, concat_axis=0, tiled=True)
        gathered = lax.all_gather(mine, "row", axis=0, tiled=True)
        picked = spread(gathered.reshape(-1, tile_width), span)
    else:
        slopes = centroid(pixels, match_filter, 1, tile_width)
        slopes = slopes.reshape(block_count, frames, tile_width)
        picked = route_start(slopes, column_order, span, tile_width, col_count)
        picked = jnp.transpose(picked, (0, 2, 1))

    chips = col_count // 2
    swap = [(d, d ^ 1) for d in range(col_count)]
    every = functools.partial(tomo, ranks=tile_ranks, picked=picked, right=right_factors, left=left_factors)
    if rows_mine == col_count:
        theirs = every(lambda m: 2 * m + 1 - own_core(), chips, dtype=BF16)
        received = lax.ppermute(theirs, "col", swap)
        ours = every(lambda m: 2 * m + own_core(), chips, dtype=F32)
    else:
        actuators = rows_mine * left_factors.shape[3] // col_count
        both = every(lambda m: m, rows_mine, dtype=F32)
        both = jnp.transpose(both, (1, 0, 2)).reshape(frames, chips, 2, actuators)
        both = jnp.transpose(both, (2, 1, 0, 3))
        theirs = lax.dynamic_index_in_dim(both, 1 - own_core(), 0, keepdims=False).astype(BF16)
        received = lax.ppermute(theirs, "col", swap)
        ours = lax.dynamic_index_in_dim(both, own_core(), 0, keepdims=False)
    out, *sends = merge(ours, received)
    for m, send in enumerate(sends):
        ahead = [(d, (d + 2 * (m + 1)) % col_count) for d in range(col_count)]
        out = out + lax.ppermute(send, "col", ahead).astype(F32)
    return out


def solution(mesh):
    in_specs = (
        P(None, ("row", "col"), None),
        P(("row", "col"), None, None),
        P("row", "col"),
        P(),
        P("row", "col", None, None),
        P("row", "col", None, None),
    )
    out_specs = P(None, ("row", "col"))
    return jax.shard_map(shards, mesh=mesh, in_specs=in_specs, out_specs=out_specs, check_vma=False)
```

```python
import functools

import jax
import jax.numpy as jnp
from jax import lax
from jax.experimental import pallas as pl
from jax.experimental.pallas import tpu as pltpu
from jax.sharding import PartitionSpec as P

F32 = jnp.float32
BF16 = jnp.bfloat16


def in_vmem(x):
    return pltpu.with_memory_space_constraint(x, pltpu.VMEM)


def in_hbm(x):
    return pltpu.with_memory_space_constraint(x, pltpu.HBM)


def limit(mib):
    return pltpu.CompilerParams(vmem_limit_bytes=mib << 20)


VMEM = pl.BlockSpec(memory_space=pltpu.VMEM)
HBM = pl.BlockSpec(memory_space=pltpu.HBM)
GROUP = 8


def centroid_kernel(pix_hbm, mf_hbm, out_ref, pix, mf, filt, xs, ys, sems, *, block_count, tile_width):
    chunk, pieces, pixel_count, width = pix_hbm.shape
    lanes = filt.shape[2]
    steps, inner, outer = pix.shape[:3]

    def fetch(step):
        if inner == chunk:
            source = pix_hbm.at[:, pl.ds(step * outer, outer)]
        else:
            source = pix_hbm.at[pl.ds(step * inner, inner), :]
        return pltpu.make_async_copy(source, pix.at[step], sems.at[step])

    fetch_mf = pltpu.make_async_copy(mf_hbm, mf, sems.at[steps])
    fetch_mf.start()
    for step in range(steps):
        fetch(step).start()
    fetch_mf.wait()
    for k in range(2):
        filt[k, :, 0:width] = mf[k].astype(F32)

    rows = 8

    @pl.loop(0, steps)
    def _(step):
        fetch(step).wait()
        f0 = pl.multiple_of(step * GROUP, GROUP)
        for lane in range(0, lanes, 128):
            w = min(128, width - lane)
            cols = slice(lane, lane + w)
            flux = [jnp.zeros((rows, w), F32) for _ in range(GROUP)]
            sx = [jnp.zeros((rows, w), F32) for _ in range(GROUP)]
            sy = [jnp.zeros((rows, w), F32) for _ in range(GROUP)]
            for p in range(0, pixel_count, rows):
                m0 = filt[0, p : p + rows, cols]
                m1 = filt[1, p : p + rows, cols]
                for f in range(GROUP):
                    v = pix[step, f % inner, f // inner, p : p + rows, cols].astype(F32)
                    flux[f] = flux[f] + v
                    sx[f] = sx[f] + v * m0
                    sy[f] = sy[f] + v * m1
            fl = jnp.concatenate([jnp.sum(a, axis=0, keepdims=True) for a in flux], axis=0)
            vx = jnp.concatenate([jnp.sum(a, axis=0, keepdims=True) for a in sx], axis=0)
            vy = jnp.concatenate([jnp.sum(a, axis=0, keepdims=True) for a in sy], axis=0)
            xs[pl.ds(f0, GROUP), cols] = vx / fl
            ys[pl.ds(f0, GROUP), cols] = vy / fl

    r = lax.broadcasted_iota(jnp.int32, (256, 256), 0)
    c = lax.broadcasted_iota(jnp.int32, (256, 256), 1)
    weave = (c == jnp.where(r < 128, 2 * r, 2 * (r - 128) + 1)).astype(BF16)
    lane_ok = lax.broadcasted_iota(jnp.int32, xs.shape, 1) < width
    x = jnp.where(lane_ok, xs[...], 0.0).astype(BF16)
    y = jnp.where(lane_ok, ys[...], 0.0).astype(BF16)
    parts = []
    for lane in range(0, lanes, 128):
        both = jnp.concatenate([x[:, lane : lane + 128], y[:, lane : lane + 128]], axis=1)
        parts.append(jnp.dot(both, weave, preferred_element_type=F32))
    woven = jnp.concatenate(parts, axis=1)
    for b in range(block_count):
        blk = woven[:, b * tile_width : (b + 1) * tile_width].astype(BF16)
        for q in range(pieces):
            out_ref[q, b * chunk : (b + 1) * chunk, :] = blk[q * chunk : (q + 1) * chunk, :]


def centroid(pixels, match_filter, pieces, tile_width):
    frames, subaps, pixel_count = pixels.shape
    chunk = frames // pieces
    inner = min(chunk, GROUP)
    assert pieces == 1 or inner == chunk
    pix = jnp.transpose(pixels, (0, 2, 1)).reshape(chunk, pieces, pixel_count, subaps)
    filt = jnp.transpose(match_filter, (1, 2, 0))
    lanes = -(-subaps // 128) * 128
    block_count = 2 * subaps // tile_width
    return pl.pallas_call(
        functools.partial(centroid_kernel, block_count=block_count, tile_width=tile_width),
        in_specs=[HBM, HBM],
        out_specs=VMEM,
        out_shape=pltpu.VMEM((pieces, block_count * chunk, tile_width), BF16),
        scratch_shapes=[
            pltpu.VMEM((frames // GROUP, inner, GROUP // inner, pixel_count, subaps), BF16),
            pltpu.VMEM((2, pixel_count, subaps), BF16),
            pltpu.VMEM((2, pixel_count, lanes), F32),
            pltpu.VMEM((frames, lanes), F32),
            pltpu.VMEM((frames, lanes), F32),
            pltpu.SemaphoreType.DMA((frames // GROUP + 1,)),
        ],
        compiler_params=limit(16),
        name="centroid",
    )(in_hbm(pix), in_hbm(filt))


def select_kernel(order_ref, in_ref, out_ref, *, block_count):
    sources, held, width = in_ref.shape
    chunk = held // block_count
    dests, rows, _ = out_ref.shape
    span = rows // chunk
    slots = order_ref.shape[1]
    shape = (sources * held, chunk * slots)
    row = lax.broadcasted_iota(jnp.int32, shape, 0)
    wanted = jnp.concatenate([order_ref[...] * chunk + f for f in range(chunk)], axis=1)
    pick = jnp.where(row == wanted, 1.0, 0.0).astype(BF16)
    out = lax.dot_general(
        pick, in_ref[...].reshape(sources * held, width), (((0,), (0,)), ((), ())), preferred_element_type=F32
    ).astype(BF16)
    for d in range(dests):
        for f in range(chunk):
            at = f * slots + d * span
            out_ref[d, f * span : (f + 1) * span, :] = out[at : at + span]


def select(order, pieces, dests, block_count):
    rows = pieces.shape[0] * pieces.shape[1] // dests
    width = pieces.shape[2]
    return pl.pallas_call(
        functools.partial(select_kernel, block_count=block_count),
        in_specs=[VMEM, VMEM],
        out_specs=VMEM,
        out_shape=pltpu.VMEM((dests, rows, width), BF16),
        compiler_params=limit(4),
        name="select",
    )(in_vmem(order.reshape(1, -1)), in_vmem(pieces))


def spread_kernel(in_ref, out_ref, wide, *, pieces):
    span, frames, width = out_ref.shape
    chunk = frames // pieces
    for n in range(wide.shape[0]):
        w = min(128, width - 128 * n)
        wide[n, :, 0:w] = in_ref[:, 128 * n : 128 * n + w].astype(F32)
        for j in range(span):
            got = [wide[n, pl.ds(f * span + j, pieces, stride=span * chunk), :] for f in range(chunk)]
            got = jnp.concatenate(got, axis=0).astype(BF16)
            out_ref[j, :, 128 * n : 128 * n + w] = got[:, 0:w]


def spread(gathered, span, pieces):
    rows, width = gathered.shape
    return pl.pallas_call(
        functools.partial(spread_kernel, pieces=pieces),
        in_specs=[VMEM],
        out_specs=VMEM,
        out_shape=pltpu.VMEM((span, rows // span, width), BF16),
        scratch_shapes=[pltpu.VMEM((-(-width // 128), rows, 128), F32)],
        compiler_params=limit(4),
        name="spread",
    )(in_vmem(gathered))


def tomo_kernel(ranks, picked_ref, right_ref, left_ref, out_ref, proj, *, pick):
    count = out_ref.shape[0]
    _, span, bound, _ = right_ref.shape
    frames = picked_ref.shape[1]
    component = lax.broadcasted_iota(jnp.int32, (bound, frames), 0)
    index = [pick(m) for m in range(count)]
    limits = [ranks[pl.ds(i, 1), :] for i in index]
    for j in range(span):
        right = jnp.concatenate([right_ref[i, j] for i in index], axis=0)
        p = lax.dot_general(right, picked_ref[j], (((1,), (1,)), ((), ())), preferred_element_type=F32)
        for m in range(count):
            q = jnp.where(component < limits[m][:, j : j + 1], p[m * bound : (m + 1) * bound], 0.0)
            proj[m, j * bound : (j + 1) * bound, :] = q.astype(BF16)
    for m, i in enumerate(index):
        left = left_ref[i].reshape(span * bound, left_ref.shape[3])
        out_ref[m] = lax.dot_general(
            proj[m], left, (((0,), (0,)), ((), ())), preferred_element_type=F32
        ).astype(out_ref.dtype)


def tomo(pick, count, ranks, picked, right, left, dtype):
    _, span, bound, _ = right.shape
    frames = picked.shape[1]
    return pl.pallas_call(
        functools.partial(tomo_kernel, pick=pick),
        in_specs=[VMEM, VMEM, VMEM, VMEM],
        out_specs=VMEM,
        out_shape=pltpu.VMEM((count, frames, left.shape[3]), dtype),
        scratch_shapes=[pltpu.VMEM((count, span * bound, frames), BF16)],
        compiler_params=limit(8),
        name="tomo",
    )(in_vmem(ranks), in_vmem(picked), in_vmem(right), in_vmem(left))


def own_core():
    return lax.rem(lax.axis_index("col"), 2)


def own_chip():
    return lax.div(lax.axis_index("col"), 2)


def ahead(m, chips):
    return lax.rem(own_chip() + m, chips)


def merge_kernel(own_ref, other_ref, *send_refs):
    for m, send in enumerate(send_refs):
        send[...] = (own_ref[m] + other_ref[m].astype(F32)).astype(BF16)


def merge(own, other):
    count, frames, width = own.shape
    return pl.pallas_call(
        merge_kernel,
        in_specs=[VMEM, VMEM],
        out_specs=[VMEM] * count,
        out_shape=[pltpu.VMEM((frames, width), BF16)] * count,
        compiler_params=limit(4),
        name="merge",
    )(in_vmem(own), in_vmem(other))


def route_start(slopes, column_order, span, tile_width, col_count):
    frame_count = slopes.shape[1]
    block_count = slopes.shape[0]
    inverse = jnp.argsort(column_order, stable=True)
    row_index = lax.axis_index("row")
    col_index = lax.axis_index("col")
    device_rank = row_index * col_count + col_index
    block_ids = device_rank * block_count + jnp.arange(block_count, dtype=jnp.int32)
    target = jnp.take(inverse, block_ids) // span
    selector = (jnp.arange(col_count, dtype=jnp.int32)[:, None] == target[None, :]).astype(BF16)
    outgoing = selector[:, :, None, None] * slopes[None]
    received = lax.all_to_all(outgoing, "col", split_axis=0, concat_axis=0, tiled=True)
    source_ids = (
        (row_index * col_count + jnp.arange(col_count, dtype=jnp.int32))[:, None] * block_count
        + jnp.arange(block_count, dtype=jnp.int32)[None, :]
    ).reshape(-1)
    local_slot = jnp.take(inverse, source_ids) - col_index * span
    placement = (jnp.arange(span, dtype=jnp.int32)[:, None] == local_slot[None, :]).astype(BF16)
    flat_blocks = received.reshape(col_count * block_count, frame_count * tile_width)
    placed = jnp.dot(placement, flat_blocks, preferred_element_type=F32)
    return lax.psum(placed.astype(BF16), "row").reshape(span, frame_count, tile_width)


def shards(pixels, match_filter, tile_ranks, column_order, right_factors, left_factors):
    frames = pixels.shape[0]
    rows_mine, span, _, tile_width = right_factors.shape
    row_count = lax.axis_size("row")
    col_count = lax.axis_size("col")
    devices = row_count * col_count
    block_count = 2 * pixels.shape[1] // tile_width

    if frames % devices == 0:
        pieces = centroid(pixels, match_filter, devices, tile_width)
        pieces = lax.all_to_all(pieces, ("row", "col"), split_axis=0, concat_axis=0, tiled=True)
        outgoing = select(column_order, pieces, col_count, block_count)
        mine = lax.all_to_all(outgoing, "col", split_axis=0, concat_axis=0, tiled=True)
        gathered = lax.all_gather(mine, "row", axis=0, tiled=True)
        picked = spread(gathered.reshape(-1, tile_width), span, devices)
    else:
        slopes = centroid(pixels, match_filter, 1, tile_width)
        slopes = slopes.reshape(block_count, frames, tile_width)
        picked = route_start(slopes, column_order, span, tile_width, col_count)

    chips = col_count // 2
    order = [chips // 2] + [m for m in range(1, chips) if m != chips // 2] + [0]
    swap = [(d, d ^ 1) for d in range(col_count)]
    every = functools.partial(tomo, ranks=tile_ranks, picked=picked, right=right_factors, left=left_factors)
    if rows_mine == col_count:
        theirs = every(lambda n: 2 * ahead(order[n], chips) + 1 - own_core(), chips, dtype=BF16)
        received = lax.ppermute(theirs, "col", swap)
        ours = every(lambda n: 2 * ahead(order[n], chips) + own_core(), chips - 1, dtype=F32)
        sends = merge(ours, received)
        out = every(lambda n: 2 * own_chip() + own_core(), 1, dtype=F32)[0]
    else:
        actuators = rows_mine * left_factors.shape[3] // col_count
        both = every(lambda n: n, rows_mine, dtype=F32)
        both = jnp.transpose(both, (1, 0, 2)).reshape(frames, chips, 2, actuators)
        both = jnp.transpose(both, (2, 1, 0, 3))
        both = jnp.take(both, jnp.stack([ahead(m, chips) for m in order]), axis=1)
        theirs = lax.dynamic_index_in_dim(both, 1 - own_core(), 0, keepdims=False).astype(BF16)
        received = lax.ppermute(theirs, "col", swap)
        ours = lax.dynamic_index_in_dim(both, own_core(), 0, keepdims=False)
        sends = merge(ours[: chips - 1], received)
        out = ours[chips - 1]
    out = out + received[chips - 1].astype(F32)
    for m, send in zip(order, sends):
        out = out + lax.ppermute(send, "col", [(d, (d + 2 * m) % col_count) for d in range(col_count)]).astype(F32)
    return out


def solution(mesh):
    in_specs = (
        P(None, ("row", "col"), None),
        P(("row", "col"), None, None),
        P("row", "col"),
        P(),
        P("row", "col", None, None),
        P("row", "col", None, None),
    )
    out_specs = P(None, ("row", "col"))
    return jax.shard_map(shards, mesh=mesh, in_specs=in_specs, out_specs=out_specs, check_vma=False)
```
